16 devices in a mesh: dp: 2 (over z), ep: 8 (over y, x, core).
Axes of the slice: x: 2, y: 2, z: 2, core: 2. Of those that a mesh axis runs over, the one named last changes fastest.
Arguments:
- hidden: bfloat16 [32768, 1024], P(('dp', 'ep'))
- grad_out: bfloat16 [32768, 1024], P(('dp', 'ep'))
- expert_ids: int32 [32768, 2], P(('dp', 'ep'))
- norm_gain: float32 [1024], replicated
- w_router: float32 [1024, 32], replicated
- w_gate: bfloat16 [32, 1024, 2816], P('ep')
- w_up: bfloat16 [32, 1024, 2816], P('ep')
- w_down: bfloat16 [32, 2816, 1024], P('ep')
Outputs:
- output 1: bfloat16 [32768, 1024], P(('dp', 'ep'))
- output 2: float32 [], replicated
- output 3: bfloat16 [32768, 1024], P(('dp', 'ep'))
- output 4: float32 [1024], replicated
- output 5: float32 [1024, 32], replicated
- output 6: bfloat16 [32, 1024, 2816], P('ep')
- output 7: bfloat16 [32, 1024, 2816], P('ep')
- output 8: bfloat16 [32, 2816, 1024], P('ep')
All inputs are finite; a program needn't handle non-finite values.
Results may differ from the reference program's by a relative error of at most 0.0146366.
Values are sent between devices in bfloat16 or wider.
A program may use at most 1 GiB of HBM per device.

```python
import functools
import jax
import jax.numpy as jnp
from jax import lax

D = 1024
FF = 2816
EXPERTS = 32
TOK = 2048
DEVICES = 16
CAP = 4 * TOK // EXPERTS
ROWS_EXP = DEVICES * CAP
S_ALL = TOK * DEVICES
EPS = 1e-6
AUX_COEF = 0.001


def draw_routes(key):
    key_order, key_shift, key_perm, key_swap = jax.random.split(key, 4)
    half_exp = EXPERTS // 2
    mean_load = 2 * TOK // EXPERTS
    shift = jax.random.randint(key_shift, (DEVICES, half_exp), 0, mean_load + 1)
    shift = shift.at[:, 0].set(mean_load)
    order = jax.vmap(lambda sub_key: jax.random.permutation(sub_key, EXPERTS))(jax.random.split(key_order, DEVICES))
    signed = jnp.concatenate([shift, -shift], axis=1)
    expert_range = jnp.arange(EXPERTS, dtype=jnp.int32)
    loads = mean_load + jnp.sum(signed[:, :, None] * (order[:, :, None] == expert_range).astype(jnp.int32), axis=1)
    bounds = jnp.cumsum(loads, axis=1)
    positions = jnp.arange(2 * TOK, dtype=jnp.int32)
    listed = jax.vmap(lambda bound_row: jnp.searchsorted(bound_row, positions, side="right"))(bounds).astype(jnp.int32)
    token_order = jax.vmap(lambda sub_key: jax.random.permutation(sub_key, TOK))(jax.random.split(key_perm, DEVICES))
    first = jnp.take_along_axis(listed[:, :TOK], token_order, axis=1)
    second = jnp.take_along_axis(listed[:, TOK:], token_order, axis=1)
    swap = jax.random.randint(key_swap, (DEVICES, TOK), 0, 2) == 1
    id_first = jnp.where(swap, second, first)
    id_second = jnp.where(swap, first, second)
    return jnp.stack([id_first, id_second], axis=-1).reshape(DEVICES * TOK, 2).astype(jnp.int32)


def setup_inputs(seed: int = 0) -> dict:
    key = jax.random.key(seed)
    keys = jax.random.split(key, 8)
    expert_ids = draw_routes(keys[0])
    w_router = jax.random.normal(keys[1], (D, EXPERTS), jnp.float32) * D ** -0.5
    col_dir = w_router * lax.rsqrt(jnp.mean(w_router * w_router, axis=0, keepdims=True))
    chosen = jnp.sum((expert_ids[:, :, None] == jnp.arange(EXPERTS, dtype=jnp.int32)).astype(jnp.float32), axis=1)
    boost = jnp.dot(chosen, col_dir.T, preferred_element_type=jnp.float32)
    hidden = jax.random.normal(keys[2], (S_ALL, D), jnp.float32) + (2.5 * D ** -0.5) * boost
    grad_out = jax.random.normal(keys[3], (S_ALL, D), jnp.float32)
    norm_gain = 1.0 + 0.3 * jax.random.normal(keys[4], (D,), jnp.float32)
    w_gate = jax.random.normal(keys[5], (EXPERTS, D, FF), jnp.float32) * D ** -0.5
    w_up = jax.random.normal(keys[6], (EXPERTS, D, FF), jnp.float32) * D ** -0.5
    w_down = jax.random.normal(keys[7], (EXPERTS, FF, D), jnp.float32) * (2.0 * FF ** -0.5)
    return {"hidden": hidden.astype(jnp.bfloat16), "grad_out": grad_out.astype(jnp.bfloat16), "expert_ids": expert_ids, "norm_gain": norm_gain, "w_router": w_router, "w_gate": w_gate.astype(jnp.bfloat16), "w_up": w_up.astype(jnp.bfloat16), "w_down": w_down.astype(jnp.bfloat16)}


def bf16_trip(value):
    return value.astype(jnp.bfloat16).astype(jnp.float32)


def route_tables(expert_ids, n_exp, capacity):
    flat_ids = expert_ids.reshape(-1)
    n_choice = flat_ids.shape[0]
    one_hot = (flat_ids[:, None] == jnp.arange(n_exp, dtype=jnp.int32)[None, :]).astype(jnp.int32)
    running = jnp.cumsum(one_hot, axis=0) - 1
    dest_rows = flat_ids * capacity + jnp.sum(running * one_hot, axis=1)
    slot_owner = jnp.full((n_exp * capacity,), n_choice, jnp.int32).at[dest_rows].set(jnp.arange(n_choice, dtype=jnp.int32))
    return dest_rows, slot_owner, jnp.sum(one_hot, axis=0)


def expert_ffn(operands):
    rows, gate_w, up_w, down_w = operands
    h_gate = bf16_trip(jnp.dot(rows, gate_w.astype(jnp.float32), preferred_element_type=jnp.float32))
    h_up = bf16_trip(jnp.dot(rows, up_w.astype(jnp.float32), preferred_element_type=jnp.float32))
    act_rows = bf16_trip(jax.nn.silu(h_gate) * h_up)
    return bf16_trip(jnp.dot(act_rows, down_w.astype(jnp.float32), preferred_element_type=jnp.float32))


def forward_pass(hidden, norm_gain, w_router, w_gate, w_up, w_down, expert_ids):
    dest_rows, slot_owner, loads = route_tables(expert_ids, EXPERTS, ROWS_EXP)
    choice_hot = (expert_ids[:, :, None] == jnp.arange(EXPERTS, dtype=jnp.int32)).astype(jnp.float32)
    x_f32 = hidden.astype(jnp.float32)
    inv_rms = lax.rsqrt(jnp.mean(x_f32 * x_f32, axis=-1, keepdims=True) + EPS)
    x_norm = bf16_trip(x_f32 * inv_rms * norm_gain)
    logits = jnp.dot(x_norm, w_router, preferred_element_type=jnp.float32)
    router_probs = jax.nn.softmax(logits, axis=-1)
    gate_vals = jnp.sum(router_probs[:, None, :] * choice_hot, axis=-1)
    rows = bf16_trip(jnp.take(x_norm, slot_owner // 2, axis=0, mode="fill", fill_value=0))
    exp_out = lax.map(jax.checkpoint(expert_ffn), (rows.reshape(EXPERTS, ROWS_EXP, D), w_gate, w_up, w_down))
    picked = jnp.take(exp_out.reshape(EXPERTS * ROWS_EXP, D), dest_rows, axis=0).reshape(S_ALL, 2, D)
    out_hidden = (x_f32 + jnp.sum(gate_vals[:, :, None] * picked, axis=1)).astype(jnp.bfloat16)
    load_frac = loads.astype(jnp.float32) / (2 * S_ALL)
    aux_loss = AUX_COEF * EXPERTS * jnp.sum(load_frac * jnp.mean(router_probs, axis=0))
    return out_hidden, aux_loss


def reference(hidden, grad_out, expert_ids, norm_gain, w_router, w_gate, w_up, w_down):
    forward_fn = functools.partial(forward_pass, expert_ids=expert_ids)
    (out_hidden, aux_loss), pullback = jax.vjp(forward_fn, hidden, norm_gain, w_router, w_gate, w_up, w_down)
    all_grads = pullback((grad_out, jnp.ones_like(aux_loss)))
    return (out_hidden, aux_loss, all_grads[0], all_grads[1], all_grads[2], all_grads[3], all_grads[4], all_grads[5])
```

```python
import functools

import jax
import jax.numpy as jnp
from jax import lax
from jax.experimental import pallas as pl
from jax.experimental.pallas import tpu as pltpu
from jax.sharding import PartitionSpec as P

EPS = 1e-6
AUX_COEF = 0.001
ROW_TILE = 256
GROUP_TILE = 512
CHUNK_ALIGN = 16
COL = 256
VMEM = 66_000_000
F32 = jnp.float32
BF16 = jnp.bfloat16


def route_tables(expert_ids, n_exp, capacity):
    flat_ids = expert_ids.reshape(-1)
    n_choice = flat_ids.shape[0]
    one_hot = (flat_ids[:, None] == jnp.arange(n_exp, dtype=jnp.int32)[None, :]).astype(jnp.int32)
    running = jnp.cumsum(one_hot, axis=0) - 1
    dest_rows = flat_ids * capacity + jnp.sum(running * one_hot, axis=1)
    slot_owner = jnp.full((n_exp * capacity,), n_choice, jnp.int32).at[dest_rows].set(jnp.arange(n_choice, dtype=jnp.int32))
    return dest_rows, slot_owner


def mm(a, b):
    return jnp.dot(a, b, preferred_element_type=F32)


def mm_t(a, b):
    return lax.dot_general(a, b, (((1,), (1,)), ((), ())), preferred_element_type=F32)


def fwd_kernel(tile_row, tile_exp, count, x_ref, wg_ref, wu_ref, wd_ref, hg_ref, hu_ref, o_ref, act_s):
    @pl.when(pl.program_id(0) < count[0])
    def _():
        ff, width = wd_ref.shape[1:]
        for j in range(ff // COL):
            cols = slice(j * COL, (j + 1) * COL)
            hg = mm(x_ref[...], wg_ref[0, :, cols]).astype(BF16)
            hu = mm(x_ref[...], wu_ref[0, :, cols]).astype(BF16)
            hg_ref[:, cols] = hg
            hu_ref[:, cols] = hu
            gate = hg.astype(F32)
            act_s[:, cols] = (gate * jax.nn.sigmoid(gate) * hu.astype(F32)).astype(BF16)
        for j in range(width // COL):
            cols = slice(j * COL, (j + 1) * COL)
            o_ref[:, cols] = mm(act_s[...], wd_ref[0, :, cols]).astype(BF16)


def gate_grads(gate, up, d_act):
    sig = jax.nn.sigmoid(gate)
    silu = gate * sig
    act = (silu * up).astype(BF16)
    d_hup = (d_act * silu).astype(BF16)
    d_hgate = (d_act * up * sig * (1.0 + gate * (1.0 - sig))).astype(BF16)
    return act, d_hgate, d_hup


def bwd_kernel(tile_row, tile_exp, count, hg_ref, hu_ref, dy_ref, w_ref, wg_ref, wu_ref, wd_ref, act_ref, dhg_ref, dhu_ref, dx_ref, do_s):
    @pl.when(pl.program_id(0) < count[0])
    def _():
        ff, width = wd_ref.shape[1:]
        do_s[...] = (dy_ref[...].astype(F32) * w_ref[...]).astype(BF16)
        for j in range(ff // COL):
            cols = slice(j * COL, (j + 1) * COL)
            d_act = mm_t(do_s[...], wd_ref[0, cols, :]).astype(BF16).astype(F32)
            act, dhg, dhu = gate_grads(hg_ref[:, cols].astype(F32), hu_ref[:, cols].astype(F32), d_act)
            act_ref[:, cols] = act
            dhg_ref[:, cols] = dhg
            dhu_ref[:, cols] = dhu
        for j in range(width // COL):
            cols = slice(j * COL, (j + 1) * COL)
            dx_ref[:, cols] = (mm_t(dhg_ref[...], wg_ref[0, cols, :]) + mm_t(dhu_ref[...], wu_ref[0, cols, :])).astype(BF16)


def both_kernel(tile_row, tile_exp, count, x_ref, dy_ref, w_ref, wg_ref, wu_ref, wd_ref, a_in, b_in, c_in, act_ref, dhg_ref, dhu_ref, do_s):
    del a_in, b_in, c_in

    @pl.when(pl.program_id(0) < count[0])
    def _():
        ff = wd_ref.shape[1]
        do_s[...] = (dy_ref[...].astype(F32) * w_ref[...]).astype(BF16)
        for j in range(ff // COL):
            cols = slice(j * COL, (j + 1) * COL)
            gate = mm(x_ref[...], wg_ref[0, :, cols]).astype(BF16).astype(F32)
            up = mm(x_ref[...], wu_ref[0, :, cols]).astype(BF16).astype(F32)
            d_act = mm_t(do_s[...], wd_ref[0, cols, :]).astype(BF16).astype(F32)
            act, dhg, dhu = gate_grads(gate, up, d_act)
            act_ref[:, cols] = act
            dhg_ref[:, cols] = dhg
            dhu_ref[:, cols] = dhu


def outer_kernel(scaled_rhs, tile_row, tile_exp, half, count, l_ref, r_ref, *refs):
    if scaled_rhs:
        w_ref, out_ref, acc, left_t, right_s = refs
    else:
        out_ref, acc, left_t = refs
    i = pl.program_id(0)
    n = count[0]
    last_step = pl.num_programs(0) - 1
    me = tile_exp[i]
    first = jnp.logical_or(i == 0, tile_exp[jnp.maximum(i - 1, 0)] != me)
    last = jnp.logical_or(i == n - 1, tile_exp[jnp.minimum(i + 1, last_step)] != me)
    live = i < n

    def add(rows):
        left_t[:, :rows] = l_ref[:rows, :].T
        if scaled_rhs:
            right_s[:rows, :] = (r_ref[:rows, :].astype(F32) * w_ref[:rows, :]).astype(BF16)
            right = right_s
        else:
            right = r_ref

        @pl.loop(0, acc.shape[1] // COL)
        def _(j):
            cols = pl.ds(pl.multiple_of(j * COL, COL), COL)
            acc[:, cols] += mm(left_t[:, :rows], right[:rows, cols])

    @pl.when(jnp.logical_and(live, first))
    def _():
        acc[...] = jnp.zeros_like(acc)

    @pl.when(jnp.logical_and(live, half[i] == 0))
    def _():
        add(GROUP_TILE)

    @pl.when(jnp.logical_and(live, half[i] == 1))
    def _():
        add(GROUP_TILE // 2)

    @pl.when(jnp.logical_and(live, last))
    def _():
        out_ref[0] = acc[...].astype(BF16)


def spread_kernel(n_chunk, rows, starts, src, dst, buf, in_sem, out_sem):
    def fetch(i):
        at = pl.multiple_of(starts[i], CHUNK_ALIGN)
        return pltpu.make_async_copy(src.at[pl.ds(at, rows), :], buf.at[i], in_sem.at[i])

    def put(i):
        return pltpu.make_async_copy(buf.at[i], dst.at[i], out_sem.at[i])

    for i in range(n_chunk):
        fetch(i).start()
    for i in range(n_chunk):
        fetch(i).wait()
        put(i).start()
    for i in range(n_chunk):
        put(i).wait()


def params():
    return pltpu.CompilerParams(dimension_semantics=("arbitrary",), vmem_limit_bytes=VMEM)


def cost(flops, nbytes):
    return pl.CostEstimate(flops=int(flops), bytes_accessed=int(nbytes), transcendentals=0)


def row_spec(cols, base=0):
    return pl.BlockSpec((ROW_TILE, cols), lambda i, r, e, c: (r[i] + base, 0))


def exp_spec(a, b):
    return pl.BlockSpec((1, a, b), lambda i, r, e, c: (e[i], 0, 0))


def solution(mesh):
    n_dp, n_ep = mesh.shape["dp"], mesh.shape["ep"]
    n_dev = n_dp * n_ep
    all_axes = ("dp", "ep")

    def local_step(hidden, grad_out, expert_ids, norm_gain, w_router, w_gate, w_up, w_down):
        n_tok, width = hidden.shape
        n_exp = w_router.shape[1]
        n_loc, _, ff = w_gate.shape
        capacity = 4 * n_tok // n_exp
        n_choice = 2 * n_tok
        total_tok = n_tok * n_dev
        half_rows = n_loc * n_ep * capacity
        my_dp, my_ep = lax.axis_index("dp"), lax.axis_index("ep")

        x_f32 = hidden.astype(F32)
        inv_rms = lax.rsqrt(jnp.mean(x_f32 * x_f32, axis=-1, keepdims=True) + EPS)
        x_hat = x_f32 * inv_rms
        x_norm = (x_hat * norm_gain).astype(BF16)
        xn_all = lax.all_gather(x_norm, all_axes, tiled=True)
        dest_rows, slot_owner = route_tables(expert_ids, n_exp, capacity)
        slots = lax.all_gather(slot_owner.reshape(n_exp, capacity), all_axes)
        dy_all = lax.all_gather(grad_out, all_axes, tiled=True)

        choice_hot = (expert_ids[:, :, None] == jnp.arange(n_exp, dtype=jnp.int32)).astype(F32)
        xn_f32 = x_norm.astype(F32)
        router_probs = jax.nn.softmax(jnp.dot(xn_f32, w_router, preferred_element_type=F32), axis=-1)
        gate_vals = jnp.sum(router_probs[:, None, :] * choice_hot, axis=-1)
        gate_slots = jnp.zeros((n_exp * capacity,), F32).at[dest_rows].set(gate_vals.reshape(-1))
        gates = lax.all_gather(gate_slots.reshape(n_exp, capacity), all_axes)
        xn_all, gates = lax.optimization_barrier((xn_all, gates))
        load_frac = jnp.sum((slots < n_choice).astype(F32), axis=(0, 2)) / (2 * total_tok)

        def mine(table):
            table = lax.dynamic_slice(table, (0, n_loc * my_ep, 0), (n_dev, n_loc, capacity))
            planes = table.reshape(n_dp, n_ep, n_loc, capacity)
            planes = jnp.where(my_dp == 0, planes, planes[::-1])
            return planes.transpose(0, 2, 1, 3)

        src_dev = (jnp.arange(n_dp)[:, None] + my_dp) % n_dp * n_ep + jnp.arange(n_ep)[None, :]
        my_slots = mine(slots)
        used = my_slots < n_choice
        load = jnp.sum(used.astype(jnp.int32), axis=-1)
        token_of = jnp.where(used, my_slots // 2 + src_dev[:, None, :, None].astype(jnp.int32) * n_tok, 0)
        room = (load + CHUNK_ALIGN - 1) // CHUNK_ALIGN * CHUNK_ALIGN
        chunk_at = jnp.cumsum(room, axis=2) - room
        group_rows = jnp.sum(room, axis=2)
        n_small = (group_rows + ROW_TILE - 1) // ROW_TILE
        n_small = jnp.maximum(n_small, jnp.array([[1], [0]], jnp.int32))
        n_big = (n_small + 1) // 2
        big_at = jnp.cumsum(n_big, axis=1) - n_big

        row = jnp.arange(half_rows, dtype=jnp.int32)
        exp_hot = (row // GROUP_TILE >= big_at[:, :, None]).astype(jnp.int32)
        exp_hot = exp_hot - jnp.concatenate([exp_hot[:, 1:], jnp.zeros_like(exp_hot[:, :1])], axis=1)
        within = row - jnp.sum(exp_hot * big_at[:, :, None], axis=1) * GROUP_TILE
        exp_of = jnp.sum(exp_hot * jnp.arange(n_loc, dtype=jnp.int32)[:, None], axis=1)
        at_row = jnp.sum(exp_hot[:, :, None, :] * chunk_at[:, :, :, None], axis=1)
        load_row = jnp.sum(exp_hot[:, :, None, :] * load[:, :, :, None], axis=1)
        src_hot = (within[:, None, :] >= at_row).astype(jnp.int32)
        src_hot = src_hot - jnp.concatenate([src_hot[:, 1:], jnp.zeros_like(src_hot[:, :1])], axis=1)
        slot = within - jnp.sum(src_hot * at_row, axis=1)
        live = slot < jnp.sum(src_hot * load_row, axis=1)
        src_of = jnp.sum(src_hot * jnp.arange(n_ep, dtype=jnp.int32)[:, None], axis=1)
        half_of = jnp.arange(n_dp, dtype=jnp.int32)[:, None]
        flat = (((half_of * n_loc + exp_of) * n_ep + src_of) * capacity + jnp.minimum(slot, capacity - 1)).reshape(-1)
        row_token = jnp.take(token_of.reshape(-1), flat, mode="clip")
        row_gate = jnp.where(live.reshape(-1), jnp.take(mine(gates).reshape(-1), flat, mode="clip"), 0.0)[:, None]

        x_rows = jnp.take(xn_all, row_token, axis=0, mode="clip")
        dy_rows = jnp.take(dy_all, row_token, axis=0, mode="clip")

        n_step = half_rows // ROW_TILE

        def small_tiles(h):
            ends = jnp.cumsum(n_small[h])
            i = jnp.minimum(jnp.arange(n_step, dtype=jnp.int32), jnp.maximum(ends[-1] - 1, 0))
            e = jnp.minimum(jnp.sum((i[None, :] >= ends[:, None]).astype(jnp.int32), axis=0), n_loc - 1)
            pick = (e[None, :] == jnp.arange(n_loc, dtype=jnp.int32)[:, None]).astype(jnp.int32)
            first = jnp.sum(pick * (2 * big_at[h] - ends + n_small[h])[:, None], axis=0)
            return first + i, e, ends[-1:]

        def big_tiles():
            n = n_big.T.reshape(-1)
            ends = jnp.cumsum(n)
            at = (big_at + jnp.arange(n_dp, dtype=jnp.int32)[:, None] * (half_rows // GROUP_TILE)).T.reshape(-1)
            i = jnp.minimum(jnp.arange(n_step, dtype=jnp.int32), ends[-1] - 1)
            q = jnp.sum((i[None, :] >= ends[:, None]).astype(jnp.int32), axis=0)
            pick = (q[None, :] == jnp.arange(n_dp * n_loc, dtype=jnp.int32)[:, None]).astype(jnp.int32)
            j = i - jnp.sum(pick * (ends - n)[:, None], axis=0)
            small = jnp.sum(pick * n_small.T.reshape(-1)[:, None], axis=0)
            return jnp.sum(pick * at[:, None], axis=0) + j, q // n_dp, (small - 2 * j < 2).astype(jnp.int32), ends[-1:]

        own_tiles, other_tiles, sum_tiles = small_tiles(0), small_tiles(1), big_tiles()
        all_rows = n_dp * half_rows
        wide = jax.ShapeDtypeStruct((all_rows, ff), BF16)
        mat_flops = half_rows * width * ff
        w_bytes = 2 * n_loc * width * ff

        h_gate, h_up, out_rows = pl.pallas_call(
            fwd_kernel,
            out_shape=(jax.ShapeDtypeStruct((half_rows, ff), BF16),) * 2 + (jax.ShapeDtypeStruct((half_rows + capacity, width), BF16),),
            grid_spec=pltpu.PrefetchScalarGridSpec(
                num_scalar_prefetch=3,
                grid=(n_step,),
                in_specs=[row_spec(width), exp_spec(width, ff), exp_spec(width, ff), exp_spec(ff, width)],
                out_specs=[row_spec(ff), row_spec(ff), row_spec(width)],
                scratch_shapes=[pltpu.VMEM((ROW_TILE, ff), BF16)],
            ),
            compiler_params=params(),
            cost_estimate=cost(3 * mat_flops, 3 * w_bytes + half_rows * (2 * ff + 2 * width)),
            name="expert_fwd",
        )(*own_tiles, x_rows, w_gate, w_up, w_down)

        n_chunk = n_ep * n_loc
        starts = (big_at[0][:, None] * GROUP_TILE + chunk_at[0]).T.reshape(-1)

        def send_back(rows, name):
            packed = pl.pallas_call(
                functools.partial(spread_kernel, n_chunk, capacity),
                out_shape=jax.ShapeDtypeStruct((n_chunk, capacity, width), BF16),
                grid_spec=pltpu.PrefetchScalarGridSpec(
                    num_scalar_prefetch=1,
                    grid=(),
                    in_specs=[pl.BlockSpec(memory_space=pl.ANY)],
                    out_specs=pl.BlockSpec(memory_space=pl.ANY),
                    scratch_shapes=[pltpu.VMEM((n_chunk, capacity, width), BF16), pltpu.SemaphoreType.DMA((n_chunk,)), pltpu.SemaphoreType.DMA((n_chunk,))],
                ),
                compiler_params=pltpu.CompilerParams(vmem_limit_bytes=VMEM),
                cost_estimate=cost(1e9, 4 * half_rows * width),
                name=name,
            )(starts, rows)
            return lax.all_to_all(packed, "ep", 0, 0, tiled=True).reshape(n_exp * capacity, width)

        back_rows = send_back(out_rows, "pack_out")

        act_rows, d_hgate, d_hup, dx_rows = pl.pallas_call(
            bwd_kernel,
            out_shape=(wide, wide, wide, jax.ShapeDtypeStruct((half_rows + capacity, width), BF16)),
            grid_spec=pltpu.PrefetchScalarGridSpec(
                num_scalar_prefetch=3,
                grid=(n_step,),
                in_specs=[row_spec(ff), row_spec(ff), row_spec(width), row_spec(1), exp_spec(width, ff), exp_spec(width, ff), exp_spec(ff, width)],
                out_specs=[row_spec(ff), row_spec(ff), row_spec(ff), row_spec(width)],
                scratch_shapes=[pltpu.VMEM((ROW_TILE, width), BF16)],
            ),
            compiler_params=params(),
            cost_estimate=cost(3 * mat_flops, 3 * w_bytes + half_rows * (5 * ff + 2 * width)),
            name="expert_bwd",
        )(*own_tiles, h_gate, h_up, dy_rows, row_gate, w_gate, w_up, w_down)

        d_back = send_back(dx_rows, "pack_dx")

        any_spec = pl.BlockSpec(memory_space=pl.ANY)
        act_rows, d_hgate, d_hup = pl.pallas_call(
            both_kernel,
            out_shape=(wide, wide, wide),
            grid_spec=pltpu.PrefetchScalarGridSpec(
                num_scalar_prefetch=3,
                grid=(n_step,),
                in_specs=[row_spec(width, n_step), row_spec(width, n_step), row_spec(1, n_step), exp_spec(width, ff), exp_spec(width, ff), exp_spec(ff, width), any_spec, any_spec, any_spec],
                out_specs=[row_spec(ff, n_step)] * 3,
                scratch_shapes=[pltpu.VMEM((ROW_TILE, width), BF16)],
            ),
            input_output_aliases={9: 0, 10: 1, 11: 2},
            compiler_params=params(),
            cost_estimate=cost(3 * mat_flops, 3 * w_bytes + half_rows * (3 * ff + 2 * width)),
            name="expert_other",
        )(*other_tiles, x_rows, dy_rows, row_gate, w_gate, w_up, w_down, act_rows, d_hgate, d_hup)

        def outer(left, right, scale, name):
            a, b = left.shape[1], right.shape[1]

            def spec(cols):
                return pl.BlockSpec((GROUP_TILE, cols), lambda i, r, e, h, c: (r[i], 0))

            scaled = scale is not None
            return pl.pallas_call(
                functools.partial(outer_kernel, scaled),
                out_shape=jax.ShapeDtypeStruct((n_loc, a, b), BF16),
                grid_spec=pltpu.PrefetchScalarGridSpec(
                    num_scalar_prefetch=4,
                    grid=(n_step,),
                    in_specs=[spec(a), spec(b)] + ([spec(1)] if scaled else []),
                    out_specs=pl.BlockSpec((1, a, b), lambda i, r, e, h, c: (e[i], 0, 0)),
                    scratch_shapes=[pltpu.VMEM((a, b), F32), pltpu.VMEM((a, GROUP_TILE), BF16)] + ([pltpu.VMEM((GROUP_TILE, b), BF16)] if scaled else []),
                ),
                compiler_params=params(),
                cost_estimate=cost(2 * mat_flops, w_bytes + all_rows * (a + b)),
                name=name,
            )(*sum_tiles, left, right, *([scale] if scaled else []))

        g_gate = outer(x_rows, d_hgate, None, "grad_gate")
        g_up = outer(x_rows, d_hup, None, "grad_up")
        g_down = outer(act_rows, dy_rows, row_gate, "grad_down")

        dest = dest_rows.reshape(n_tok, 2)
        picked = [jnp.take(back_rows, dest[:, j], axis=0, mode="clip").astype(F32) for j in range(2)]
        out_hidden = (x_f32 + (gate_vals[:, :1] * picked[0] + gate_vals[:, 1:] * picked[1])).astype(BF16)
        dy_f32 = grad_out.astype(F32)
        d_gates = [jnp.sum(dy_f32 * p, axis=-1, keepdims=True) for p in picked]
        d_probs = d_gates[0] * choice_hot[:, 0] + d_gates[1] * choice_hot[:, 1] + (AUX_COEF * n_exp / total_tok) * load_frac
        d_logits = router_probs * (d_probs - jnp.sum(router_probs * d_probs, axis=-1, keepdims=True))
        d_taken = [jnp.take(d_back, dest[:, j], axis=0, mode="clip").astype(F32) for j in range(2)]
        d_xnorm = jnp.einsum("te,de->td", d_logits, w_router) + d_taken[0] + d_taken[1]
        d_xnorm = d_xnorm.astype(BF16).astype(F32)
        scaled = d_xnorm * norm_gain
        grad_hidden = (inv_rms * (scaled - x_hat * jnp.mean(scaled * x_hat, axis=-1, keepdims=True)) + dy_f32).astype(BF16)
        prob_sum, g_gain, g_router = lax.psum((jnp.sum(router_probs, axis=0), jnp.sum(d_xnorm * x_hat, axis=0), jnp.einsum("td,te->de", xn_f32, d_logits)), all_axes)
        aux_loss = AUX_COEF * n_exp * jnp.sum(load_frac * prob_sum / total_tok)
        return (out_hidden, aux_loss, grad_hidden, g_gain, g_router, g_gate, g_up, g_down)

    tok_spec = P(all_axes, None)
    w_spec = P("ep", None, None)
    return jax.shard_map(local_step, mesh=mesh, in_specs=(tok_spec, tok_spec, tok_spec, P(), P(), w_spec, w_spec, w_spec), out_specs=(tok_spec, P(), tok_spec, P(), P(), w_spec, w_spec, w_spec), check_vma=False)
```

```python
import functools

import jax
import jax.numpy as jnp
from jax import lax
from jax.experimental import pallas as pl
from jax.experimental.pallas import tpu as pltpu
from jax.sharding import PartitionSpec as P

EPS = 1e-6
AUX_COEF = 0.001
ROW_TILE = 256
GROUP_TILE = 512
CHUNK_ALIGN = 16
COL = 256
VMEM = 66_000_000
F32 = jnp.float32
BF16 = jnp.bfloat16


def route_tables(expert_ids, n_exp, capacity):
    flat_ids = expert_ids.reshape(-1)
    n_choice = flat_ids.shape[0]
    one_hot = (flat_ids[:, None] == jnp.arange(n_exp, dtype=jnp.int32)[None, :]).astype(jnp.int32)
    running = jnp.cumsum(one_hot, axis=0) - 1
    dest_rows = flat_ids * capacity + jnp.sum(running * one_hot, axis=1)
    slot_owner = jnp.full((n_exp * capacity,), n_choice, jnp.int32).at[dest_rows].set(jnp.arange(n_choice, dtype=jnp.int32))
    return dest_rows, slot_owner


def mm(a, b):
    return jnp.dot(a, b, preferred_element_type=F32)


def mm_t(a, b):
    return lax.dot_general(a, b, (((1,), (1,)), ((), ())), preferred_element_type=F32)


def pieces(rows, make):
    size = ROW_TILE
    while size >= CHUNK_ALIGN:

        @pl.when(rows & size != 0)
        def _(size=size):
            make(pl.multiple_of(rows & ~(2 * size - 1), CHUNK_ALIGN), size)

        size //= 2


def pack_kernel(scaled, n_loc, src_dev, row_at, room, zero_at, zero_rows, tok_ref, *refs):
    if scaled:
        gate_ref, src_ref, out, hot, buf, zeros, sem, zero_sem = refs
    else:
        src_ref, out, hot, buf, zeros, sem, zero_sem = refs
    step, n_step = pl.program_id(0), pl.num_programs(0)
    n_tok, width = src_ref.shape
    capacity = tok_ref.shape[2]

    def put(k, slot, wait):
        at = pl.multiple_of(row_at[k], CHUNK_ALIGN)

        def one(off, size):
            copy = pltpu.make_async_copy(buf.at[slot, pl.ds(off, size), :], out.at[pl.ds(at + off, size), :], sem.at[slot])
            copy.wait() if wait else copy.start()

        pieces(room[k], one)

    def fill(wait):
        for g in range(zero_at.shape[0]):
            at = pl.multiple_of(zero_at[g], CHUNK_ALIGN)

            def one(off, size, at=at):
                copy = pltpu.make_async_copy(zeros.at[pl.ds(0, size), :], out.at[pl.ds(at + off, size), :], zero_sem)
                copy.wait() if wait else copy.start()

            pieces(zero_rows[g], one)

    @pl.when(step == 0)
    def _():
        zeros[...] = jnp.zeros_like(zeros)
        fill(False)

    def pick(e, slot, rows):
        tok = tok_ref[0, e, :rows, :]
        for j in range(n_tok // COL):
            lane = lax.broadcasted_iota(jnp.int32, (rows, COL), 1) + j * COL
            hot[:rows, j * COL : (j + 1) * COL] = jnp.where(tok == lane, 1.0, 0.0).astype(BF16)
        for j in range(width // COL):
            cols = slice(j * COL, (j + 1) * COL)
            got = mm(hot[:rows, :], src_ref[:, cols])
            if scaled:
                got = got * gate_ref[0, e, :rows, :]
            buf[slot, :rows, cols] = got.astype(BF16)

    @pl.loop(0, n_loc)
    def _(e):
        k = step * n_loc + e
        slot = k % 2

        @pl.when(k >= 2)
        def _():
            put(jnp.maximum(k - 2, 0), slot, True)

        @pl.when(room[k] > capacity // 2)
        def _():
            pick(e, slot, capacity)

        @pl.when(jnp.logical_and(room[k] > 0, room[k] <= capacity // 2))
        def _():
            pick(e, slot, capacity // 2)

        put(k, slot, False)

    @pl.when(step == n_step - 1)
    def _():
        last = n_step * n_loc - 1
        put(last - 1, (last - 1) % 2, True)
        put(last, last % 2, True)
        fill(True)


def fwd_kernel(tile_row, tile_exp, count, x_ref, wg_ref, wu_ref, wd_ref, hg_ref, hu_ref, o_ref, act_s):
    @pl.when(pl.program_id(0) < count[0])
    def _():
        ff, width = wd_ref.shape[1:]
        for j in range(ff // COL):
            cols = slice(j * COL, (j + 1) * COL)
            hg = mm(x_ref[...], wg_ref[0, :, cols]).astype(BF16)
            hu = mm(x_ref[...], wu_ref[0, :, cols]).astype(BF16)
            hg_ref[:, cols] = hg
            hu_ref[:, cols] = hu
            gate = hg.astype(F32)
            act_s[:, cols] = (gate * jax.nn.sigmoid(gate) * hu.astype(F32)).astype(BF16)
        for j in range(width // COL):
            cols = slice(j * COL, (j + 1) * COL)
            o_ref[:, cols] = mm(act_s[...], wd_ref[0, :, cols]).astype(BF16)


def gate_grads(gate, up, d_act):
    sig = jax.nn.sigmoid(gate)
    silu = gate * sig
    act = (silu * up).astype(BF16)
    d_hup = (d_act * silu).astype(BF16)
    d_hgate = (d_act * up * sig * (1.0 + gate * (1.0 - sig))).astype(BF16)
    return act, d_hgate, d_hup


def bwd_kernel(tile_row, tile_exp, count, hg_ref, hu_ref, do_ref, wg_ref, wu_ref, wd_ref, act_ref, dhg_ref, dhu_ref, dx_ref):
    @pl.when(pl.program_id(0) < count[0])
    def _():
        ff, width = wd_ref.shape[1:]
        for j in range(ff // COL):
            cols = slice(j * COL, (j + 1) * COL)
            d_act = mm_t(do_ref[...], wd_ref[0, cols, :]).astype(BF16).astype(F32)
            act, dhg, dhu = gate_grads(hg_ref[:, cols].astype(F32), hu_ref[:, cols].astype(F32), d_act)
            act_ref[:, cols] = act
            dhg_ref[:, cols] = dhg
            dhu_ref[:, cols] = dhu
        for j in range(width // COL):
            cols = slice(j * COL, (j + 1) * COL)
            dx_ref[:, cols] = (mm_t(dhg_ref[...], wg_ref[0, cols, :]) + mm_t(dhu_ref[...], wu_ref[0, cols, :])).astype(BF16)


def both_kernel(tile_row, tile_exp, count, x_ref, do_ref, wg_ref, wu_ref, wd_ref, a_in, b_in, c_in, act_ref, dhg_ref, dhu_ref):
    del a_in, b_in, c_in

    @pl.when(pl.program_id(0) < count[0])
    def _():
        ff = wd_ref.shape[1]
        for j in range(ff // COL):
            cols = slice(j * COL, (j + 1) * COL)
            gate = mm(x_ref[...], wg_ref[0, :, cols]).astype(BF16).astype(F32)
            up = mm(x_ref[...], wu_ref[0, :, cols]).astype(BF16).astype(F32)
            d_act = mm_t(do_ref[...], wd_ref[0, cols, :]).astype(BF16).astype(F32)
            act, dhg, dhu = gate_grads(gate, up, d_act)
            act_ref[:, cols] = act
            dhg_ref[:, cols] = dhg
            dhu_ref[:, cols] = dhu


def outer_kernel(tile_row, tile_exp, half, count, l_ref, r_ref, out_ref, acc, left_t):
    i = pl.program_id(0)
    n = count[0]
    last_step = pl.num_programs(0) - 1
    me = tile_exp[i]
    first = jnp.logical_or(i == 0, tile_exp[jnp.maximum(i - 1, 0)] != me)
    last = jnp.logical_or(i == n - 1, tile_exp[jnp.minimum(i + 1, last_step)] != me)
    live = i < n

    def add(rows):
        left_t[:, :rows] = l_ref[:rows, :].T
        for j in range(acc.shape[1] // COL):
            cols = slice(j * COL, (j + 1) * COL)
            acc[:, cols] += mm(left_t[:, :rows], r_ref[:rows, cols])

    @pl.when(jnp.logical_and(live, first))
    def _():
        acc[...] = jnp.zeros_like(acc)

    @pl.when(jnp.logical_and(live, half[i] == 0))
    def _():
        add(GROUP_TILE)

    @pl.when(jnp.logical_and(live, half[i] == 1))
    def _():
        add(GROUP_TILE // 2)

    @pl.when(jnp.logical_and(live, last))
    def _():
        out_ref[0] = acc[...].astype(BF16)


def spread_kernel(n_chunk, rows, starts, src, dst, buf, in_sem, out_sem):
    def fetch(i):
        at = pl.multiple_of(starts[i], CHUNK_ALIGN)
        return pltpu.make_async_copy(src.at[pl.ds(at, rows), :], buf.at[i], in_sem.at[i])

    def put(i):
        return pltpu.make_async_copy(buf.at[i], dst.at[i], out_sem.at[i])

    for i in range(n_chunk):
        fetch(i).start()
    for i in range(n_chunk):
        fetch(i).wait()
        put(i).start()
    for i in range(n_chunk):
        put(i).wait()


def params():
    return pltpu.CompilerParams(dimension_semantics=("arbitrary",), vmem_limit_bytes=VMEM)


def cost(flops, nbytes):
    return pl.CostEstimate(flops=int(flops), bytes_accessed=int(nbytes), transcendentals=0)


def row_spec(cols, base=0):
    return pl.BlockSpec((ROW_TILE, cols), lambda i, r, e, c: (r[i] + base, 0))


def exp_spec(a, b):
    return pl.BlockSpec((1, a, b), lambda i, r, e, c: (e[i], 0, 0))


def solution(mesh):
    n_dp, n_ep = mesh.shape["dp"], mesh.shape["ep"]
    n_dev = n_dp * n_ep
    all_axes = ("dp", "ep")

    def local_step(hidden, grad_out, expert_ids, norm_gain, w_router, w_gate, w_up, w_down):
        n_tok, width = hidden.shape
        n_exp = w_router.shape[1]
        n_loc, _, ff = w_gate.shape
        capacity = 4 * n_tok // n_exp
        n_choice = 2 * n_tok
        total_tok = n_tok * n_dev
        half_rows = n_loc * n_ep * capacity
        my_dp, my_ep = lax.axis_index("dp"), lax.axis_index("ep")

        x_f32 = hidden.astype(F32)
        inv_rms = lax.rsqrt(jnp.mean(x_f32 * x_f32, axis=-1, keepdims=True) + EPS)
        x_hat = x_f32 * inv_rms
        x_norm = (x_hat * norm_gain).astype(BF16)
        xn_all = lax.all_gather(x_norm, all_axes, tiled=True)
        dest_rows, slot_owner = route_tables(expert_ids, n_exp, capacity)
        slots = lax.all_gather(slot_owner.reshape(n_exp, capacity), all_axes)
        dy_all = lax.all_gather(grad_out, all_axes, tiled=True)

        choice_hot = (expert_ids[:, :, None] == jnp.arange(n_exp, dtype=jnp.int32)).astype(F32)
        xn_f32 = x_norm.astype(F32)
        router_probs = jax.nn.softmax(jnp.dot(xn_f32, w_router, preferred_element_type=F32), axis=-1)
        gate_vals = jnp.sum(router_probs[:, None, :] * choice_hot, axis=-1)
        gate_slots = jnp.zeros((n_exp * capacity,), F32).at[dest_rows].set(gate_vals.reshape(-1))
        gates = lax.all_gather(gate_slots.reshape(n_exp, capacity), all_axes)
        load_frac = jnp.sum((slots < n_choice).astype(F32), axis=(0, 2)) / (2 * total_tok)

        def mine(table):
            table = lax.dynamic_slice(table, (0, n_loc * my_ep, 0), (n_dev, n_loc, capacity))
            planes = table.reshape(n_dp, n_ep, n_loc, capacity)
            return jnp.where(my_dp == 0, planes, planes[::-1])

        src_dev = ((jnp.arange(n_dp)[:, None] + my_dp) % n_dp * n_ep + jnp.arange(n_ep)[None, :]).astype(jnp.int32)
        my_slots = mine(slots)
        load = jnp.sum((my_slots < n_choice).astype(jnp.int32), axis=-1).transpose(0, 2, 1)
        room = (load + CHUNK_ALIGN - 1) // CHUNK_ALIGN * CHUNK_ALIGN
        chunk_at = jnp.cumsum(room, axis=2) - room
        group_rows = jnp.sum(room, axis=2)
        n_small = (group_rows + ROW_TILE - 1) // ROW_TILE
        n_small = jnp.maximum(n_small, jnp.array([[1], [0]], jnp.int32))
        n_big = (n_small + 1) // 2
        big_at = jnp.cumsum(n_big, axis=1) - n_big
        group_at = big_at * GROUP_TILE + jnp.arange(n_dp, dtype=jnp.int32)[:, None] * half_rows
        row_at = (group_at[:, :, None] + chunk_at).transpose(0, 2, 1).reshape(-1)
        pack_lists = (src_dev.reshape(-1), row_at, room.transpose(0, 2, 1).reshape(-1), (group_at + group_rows).reshape(-1), (n_small * ROW_TILE - group_rows).reshape(-1))
        slot_token = (my_slots // 2).reshape(n_dev, n_loc, capacity, 1)

        def pack(lists, table, gate, name):
            scaled = gate is not None
            col_spec = pl.BlockSpec((1, n_loc, capacity, 1), lambda i, *_: (i, 0, 0, 0))
            return pl.pallas_call(
                functools.partial(pack_kernel, scaled, n_loc),
                out_shape=jax.ShapeDtypeStruct((n_dp * half_rows, width), BF16),
                grid_spec=pltpu.PrefetchScalarGridSpec(
                    num_scalar_prefetch=5,
                    grid=(n_dev,),
                    in_specs=[col_spec] * (1 + scaled) + [pl.BlockSpec((n_tok, width), lambda i, s, *_: (s[i], 0))],
                    out_specs=pl.BlockSpec(memory_space=pl.ANY),
                    scratch_shapes=[
                        pltpu.VMEM((ROW_TILE, n_tok), BF16),
                        pltpu.VMEM((2, ROW_TILE, width), BF16),
                        pltpu.VMEM((ROW_TILE, width), BF16),
                        pltpu.SemaphoreType.DMA((2,)),
                        pltpu.SemaphoreType.DMA,
                    ],
                ),
                compiler_params=params(),
                cost_estimate=cost(2 * n_dev * n_loc * capacity * n_tok * width, 2 * n_dev * n_tok * width),
                name=name,
            )(*lists, slot_token, *([gate] if scaled else []), table)

        slot_gate = mine(gates).reshape(n_dev, n_loc, capacity, 1)
        early = lax.optimization_barrier((pack_lists[1], slot_gate))
        x_rows = pack((pack_lists[0], early[0], *pack_lists[2:]), xn_all, None, "pack_x")
        do_rows = pack(pack_lists, dy_all, early[1], "pack_do")

        n_step = half_rows // ROW_TILE

        def small_tiles(h):
            ends = jnp.cumsum(n_small[h])
            i = jnp.minimum(jnp.arange(n_step, dtype=jnp.int32), jnp.maximum(ends[-1] - 1, 0))
            e = jnp.minimum(jnp.sum((i[None, :] >= ends[:, None]).astype(jnp.int32), axis=0), n_loc - 1)
            pick = (e[None, :] == jnp.arange(n_loc, dtype=jnp.int32)[:, None]).astype(jnp.int32)
            first = jnp.sum(pick * (2 * big_at[h] - ends + n_small[h])[:, None], axis=0)
            return first + i, e, ends[-1:]

        def big_tiles():
            n = n_big.T.reshape(-1)
            ends = jnp.cumsum(n)
            at = (big_at + jnp.arange(n_dp, dtype=jnp.int32)[:, None] * (half_rows // GROUP_TILE)).T.reshape(-1)
            i = jnp.minimum(jnp.arange(n_step, dtype=jnp.int32), ends[-1] - 1)
            q = jnp.sum((i[None, :] >= ends[:, None]).astype(jnp.int32), axis=0)
            pick = (q[None, :] == jnp.arange(n_dp * n_loc, dtype=jnp.int32)[:, None]).astype(jnp.int32)
            j = i - jnp.sum(pick * (ends - n)[:, None], axis=0)
            small = jnp.sum(pick * n_small.T.reshape(-1)[:, None], axis=0)
            return jnp.sum(pick * at[:, None], axis=0) + j, q // n_dp, (small - 2 * j < 2).astype(jnp.int32), ends[-1:]

        own_tiles, other_tiles, sum_tiles = small_tiles(0), small_tiles(1), big_tiles()
        all_rows = n_dp * half_rows
        wide = jax.ShapeDtypeStruct((all_rows, ff), BF16)
        mat_flops = half_rows * width * ff
        w_bytes = 2 * n_loc * width * ff

        h_gate, h_up, out_rows = pl.pallas_call(
            fwd_kernel,
            out_shape=(jax.ShapeDtypeStruct((half_rows, ff), BF16),) * 2 + (jax.ShapeDtypeStruct((half_rows + capacity, width), BF16),),
            grid_spec=pltpu.PrefetchScalarGridSpec(
                num_scalar_prefetch=3,
                grid=(n_step,),
                in_specs=[row_spec(width), exp_spec(width, ff), exp_spec(width, ff), exp_spec(ff, width)],
                out_specs=[row_spec(ff), row_spec(ff), row_spec(width)],
                scratch_shapes=[pltpu.VMEM((ROW_TILE, ff), BF16)],
            ),
            compiler_params=params(),
            cost_estimate=cost(3 * mat_flops, 3 * w_bytes + half_rows * (2 * ff + 2 * width)),
            name="expert_fwd",
        )(*own_tiles, x_rows, w_gate, w_up, w_down)

        n_chunk = n_ep * n_loc
        starts = (big_at[0][:, None] * GROUP_TILE + chunk_at[0]).T.reshape(-1)

        def send_back(rows, name):
            packed = pl.pallas_call(
                functools.partial(spread_kernel, n_chunk, capacity),
                out_shape=jax.ShapeDtypeStruct((n_chunk, capacity, width), BF16),
                grid_spec=pltpu.PrefetchScalarGridSpec(
                    num_scalar_prefetch=1,
                    grid=(),
                    in_specs=[pl.BlockSpec(memory_space=pl.ANY)],
                    out_specs=pl.BlockSpec(memory_space=pl.ANY),
                    scratch_shapes=[pltpu.VMEM((n_chunk, capacity, width), BF16), pltpu.SemaphoreType.DMA((n_chunk,)), pltpu.SemaphoreType.DMA((n_chunk,))],
                ),
                compiler_params=pltpu.CompilerParams(vmem_limit_bytes=VMEM),
                cost_estimate=cost(1e9, 4 * half_rows * width),
                name=name,
            )(starts, rows)
            return lax.all_to_all(packed, "ep", 0, 0, tiled=True).reshape(n_exp * capacity, width)

        back_rows = send_back(out_rows, "pack_out")

        act_rows, d_hgate, d_hup, dx_rows = pl.pallas_call(
            bwd_kernel,
            out_shape=(wide, wide, wide, jax.ShapeDtypeStruct((half_rows + capacity, width), BF16)),
            grid_spec=pltpu.PrefetchScalarGridSpec(
                num_scalar_prefetch=3,
                grid=(n_step,),
                in_specs=[row_spec(ff), row_spec(ff), row_spec(width), exp_spec(width, ff), exp_spec(width, ff), exp_spec(ff, width)],
                out_specs=[row_spec(ff), row_spec(ff), row_spec(ff), row_spec(width)],
            ),
            compiler_params=params(),
            cost_estimate=cost(3 * mat_flops, 3 * w_bytes + half_rows * (5 * ff + 2 * width)),
            name="expert_bwd",
        )(*own_tiles, h_gate, h_up, do_rows, w_gate, w_up, w_down)

        d_back = send_back(dx_rows, "pack_dx")

        any_spec = pl.BlockSpec(memory_space=pl.ANY)
        act_rows, d_hgate, d_hup = pl.pallas_call(
            both_kernel,
            out_shape=(wide, wide, wide),
            grid_spec=pltpu.PrefetchScalarGridSpec(
                num_scalar_prefetch=3,
                grid=(n_step,),
                in_specs=[row_spec(width, n_step), row_spec(width, n_step), exp_spec(width, ff), exp_spec(width, ff), exp_spec(ff, width), any_spec, any_spec, any_spec],
                out_specs=[row_spec(ff, n_step)] * 3,
            ),
            input_output_aliases={8: 0, 9: 1, 10: 2},
            compiler_params=params(),
            cost_estimate=cost(3 * mat_flops, 3 * w_bytes + half_rows * (3 * ff + 2 * width)),
            name="expert_other",
        )(*other_tiles, x_rows, do_rows, w_gate, w_up, w_down, act_rows, d_hgate, d_hup)

        def outer(tiles, left, right, name):
            a, b = left.shape[1], right.shape[1]

            def spec(cols):
                return pl.BlockSpec((GROUP_TILE, cols), lambda i, r, e, h, c: (r[i], 0))

            return pl.pallas_call(
                outer_kernel,
                out_shape=jax.ShapeDtypeStruct((n_loc, a, b), BF16),
                grid_spec=pltpu.PrefetchScalarGridSpec(
                    num_scalar_prefetch=4,
                    grid=(n_step,),
                    in_specs=[spec(a), spec(b)],
                    out_specs=pl.BlockSpec((1, a, b), lambda i, r, e, h, c: (e[i], 0, 0)),
                    scratch_shapes=[pltpu.VMEM((a, b), F32), pltpu.VMEM((a, GROUP_TILE), BF16)],
                ),
                compiler_params=params(),
                cost_estimate=cost(2 * mat_flops, w_bytes + all_rows * (a + b)),
                name=name,
            )(*tiles, left, right)

        g_down = outer(sum_tiles, act_rows, do_rows, "grad_down")

        dest = dest_rows.reshape(n_tok, 2)
        picked = [jnp.take(back_rows, dest[:, j], axis=0, mode="clip").astype(F32) for j in range(2)]
        out_hidden = (x_f32 + (gate_vals[:, :1] * picked[0] + gate_vals[:, 1:] * picked[1])).astype(BF16)
        dy_f32 = grad_out.astype(F32)
        d_gates = [jnp.sum(dy_f32 * p, axis=-1, keepdims=True) for p in picked]
        d_probs = d_gates[0] * choice_hot[:, 0] + d_gates[1] * choice_hot[:, 1] + (AUX_COEF * n_exp / total_tok) * load_frac
        d_logits = router_probs * (d_probs - jnp.sum(router_probs * d_probs, axis=-1, keepdims=True))
        d_taken = [jnp.take(d_back, dest[:, j], axis=0, mode="clip").astype(F32) for j in range(2)]
        d_xnorm = jnp.einsum("te,de->td", d_logits, w_router) + d_taken[0] + d_taken[1]
        d_xnorm = d_xnorm.astype(BF16).astype(F32)
        scaled = d_xnorm * norm_gain
        grad_hidden = (inv_rms * (scaled - x_hat * jnp.mean(scaled * x_hat, axis=-1, keepdims=True)) + dy_f32).astype(BF16)
        g_gain = jnp.sum(d_xnorm * x_hat, axis=0)
        g_router = jnp.einsum("td,te->de", xn_f32, d_logits)
        prob_sum = jnp.pad(jnp.sum(router_probs, axis=0), (0, width - n_exp))
        count, small_sums = lax.optimization_barrier((sum_tiles[3], jnp.concatenate([g_router, g_gain[:, None], prob_sum[:, None]], axis=1)))
        small_sums = lax.psum(small_sums, all_axes)
        g_router, g_gain, prob_sum = small_sums[:, :n_exp], small_sums[:, n_exp], small_sums[:n_exp, n_exp + 1]
        g_gate = outer((*sum_tiles[:3], count), x_rows, d_hgate, "grad_gate")
        g_up = outer((*sum_tiles[:3], count), x_rows, d_hup, "grad_up")
        aux_loss = AUX_COEF * n_exp * jnp.sum(load_frac * prob_sum / total_tok)
        return (out_hidden, aux_loss, grad_hidden, g_gain, g_router, g_gate, g_up, g_down)

    tok_spec = P(all_axes, None)
    w_spec = P("ep", None, None)
    return jax.shard_map(local_step, mesh=mesh, in_specs=(tok_spec, tok_spec, tok_spec, P(), P(), w_spec, w_spec, w_spec), out_specs=(tok_spec, P(), tok_spec, P(), P(), w_spec, w_spec, w_spec), check_vma=False)
```

```python
import functools

import jax
import jax.numpy as jnp
from jax import lax
from jax.experimental import pallas as pl
from jax.experimental.pallas import tpu as pltpu
from jax.sharding import PartitionSpec as P

EPS = 1e-6
AUX_COEF = 0.001
ROW_TILE = 256
GROUP_TILE = 512
CHUNK_ALIGN = 16
COL = 256
VMEM = 66_000_000
F32 = jnp.float32
BF16 = jnp.bfloat16


def route_tables(expert_ids, n_exp, capacity):
    flat_ids = expert_ids.reshape(-1)
    n_choice = flat_ids.shape[0]
    one_hot = (flat_ids[:, None] == jnp.arange(n_exp, dtype=jnp.int32)[None, :]).astype(jnp.int32)
    running = jnp.cumsum(one_hot, axis=0) - 1
    dest_rows = flat_ids * capacity + jnp.sum(running * one_hot, axis=1)
    slot_owner = jnp.full((n_exp * capacity,), n_choice, jnp.int32).at[dest_rows].set(jnp.arange(n_choice, dtype=jnp.int32))
    return dest_rows, slot_owner


def mm(a, b):
    return jnp.dot(a, b, preferred_element_type=F32)


def mm_t(a, b):
    return lax.dot_general(a, b, (((1,), (1,)), ((), ())), preferred_element_type=F32)


def pieces(rows, make):
    size = ROW_TILE
    while size >= CHUNK_ALIGN:

        @pl.when(rows & size != 0)
        def _(size=size):
            make(pl.multiple_of(rows & ~(2 * size - 1), CHUNK_ALIGN), size)

        size //= 2


def pack_kernel(scaled, carry, n_loc, src_dev, row_at, room, zero_at, zero_rows, tok_ref, *refs):
    gate_ref = refs[0]
    src_ref = refs[scaled]
    out, hot, buf, zeros, sem, zero_sem = refs[scaled + 1 + carry :]
    step, n_step = pl.program_id(0), pl.num_programs(0)
    n_tok, width = src_ref.shape
    capacity = tok_ref.shape[2]

    def put(k, slot, wait):
        at = pl.multiple_of(row_at[k], CHUNK_ALIGN)

        def one(off, size):
            copy = pltpu.make_async_copy(buf.at[slot, pl.ds(off, size), :], out.at[pl.ds(at + off, size), :], sem.at[slot])
            copy.wait() if wait else copy.start()

        pieces(room[k], one)

    def fill(wait):
        for g in range(zero_at.shape[0]):
            at = pl.multiple_of(zero_at[g], CHUNK_ALIGN)

            def one(off, size, at=at):
                copy = pltpu.make_async_copy(zeros.at[pl.ds(0, size), :], out.at[pl.ds(at + off, size), :], zero_sem)
                copy.wait() if wait else copy.start()

            pieces(zero_rows[g], one)

    @pl.when(step == 0)
    def _():
        zeros[...] = jnp.zeros_like(zeros)
        fill(False)

    def pick(e, slot, rows):
        tok = tok_ref[0, e, :rows, :]
        for j in range(n_tok // COL):
            lane = lax.broadcasted_iota(jnp.int32, (rows, COL), 1) + j * COL
            hot[:rows, j * COL : (j + 1) * COL] = jnp.where(tok == lane, 1.0, 0.0).astype(BF16)
        for j in range(width // COL):
            cols = slice(j * COL, (j + 1) * COL)
            got = mm(hot[:rows, :], src_ref[:, cols])
            if scaled:
                got = got * gate_ref[0, e, :rows, :]
            buf[slot, :rows, cols] = got.astype(BF16)

    @pl.loop(0, n_loc)
    def _(e):
        k = step * n_loc + e
        slot = k % 2

        @pl.when(k >= 2)
        def _():
            put(jnp.maximum(k - 2, 0), slot, True)

        @pl.when(room[k] > capacity // 2)
        def _():
            pick(e, slot, capacity)

        @pl.when(jnp.logical_and(room[k] > 0, room[k] <= capacity // 2))
        def _():
            pick(e, slot, capacity // 2)

        put(k, slot, False)

    @pl.when(step == n_step - 1)
    def _():
        last = n_step * n_loc - 1
        put(last - 1, (last - 1) % 2, True)
        put(last, last % 2, True)
        fill(True)


def fwd_kernel(tile_row, tile_exp, count, x_ref, wg_ref, wu_ref, wd_ref, hg_ref, hu_ref, o_ref, act_s):
    @pl.when(pl.program_id(0) < count[0])
    def _():
        ff, width = wd_ref.shape[1:]
        for j in range(ff // COL):
            cols = slice(j * COL, (j + 1) * COL)
            hg = mm(x_ref[...], wg_ref[0, :, cols]).astype(BF16)
            hu = mm(x_ref[...], wu_ref[0, :, cols]).astype(BF16)
            hg_ref[:, cols] = hg
            hu_ref[:, cols] = hu
            gate = hg.astype(F32)
            act_s[:, cols] = (gate * jax.nn.sigmoid(gate) * hu.astype(F32)).astype(BF16)
        for j in range(width // COL):
            cols = slice(j * COL, (j + 1) * COL)
            o_ref[:, cols] = mm(act_s[...], wd_ref[0, :, cols]).astype(BF16)


def gate_grads(gate, up, d_act):
    sig = jax.nn.sigmoid(gate)
    silu = gate * sig
    act = (silu * up).astype(BF16)
    d_hup = (d_act * silu).astype(BF16)
    d_hgate = (d_act * up * sig * (1.0 + gate * (1.0 - sig))).astype(BF16)
    return act, d_hgate, d_hup


def bwd_kernel(tile_row, tile_exp, count, hg_ref, hu_ref, do_ref, wg_ref, wu_ref, wd_ref, act_ref, dhg_ref, dhu_ref, dx_ref):
    @pl.when(pl.program_id(0) < count[0])
    def _():
        ff, width = wd_ref.shape[1:]
        for j in range(ff // COL):
            cols = slice(j * COL, (j + 1) * COL)
            d_act = mm_t(do_ref[...], wd_ref[0, cols, :]).astype(BF16).astype(F32)
            act, dhg, dhu = gate_grads(hg_ref[:, cols].astype(F32), hu_ref[:, cols].astype(F32), d_act)
            act_ref[:, cols] = act
            dhg_ref[:, cols] = dhg
            dhu_ref[:, cols] = dhu
        for j in range(width // COL):
            cols = slice(j * COL, (j + 1) * COL)
            dx_ref[:, cols] = (mm_t(dhg_ref[...], wg_ref[0, cols, :]) + mm_t(dhu_ref[...], wu_ref[0, cols, :])).astype(BF16)


def both_kernel(tile_row, tile_exp, count, x_ref, do_ref, wg_ref, wu_ref, wd_ref, a_in, b_in, c_in, act_ref, dhg_ref, dhu_ref):
    del a_in, b_in, c_in

    @pl.when(pl.program_id(0) < count[0])
    def _():
        ff = wd_ref.shape[1]
        for j in range(ff // COL):
            cols = slice(j * COL, (j + 1) * COL)
            gate = mm(x_ref[...], wg_ref[0, :, cols]).astype(BF16).astype(F32)
            up = mm(x_ref[...], wu_ref[0, :, cols]).astype(BF16).astype(F32)
            d_act = mm_t(do_ref[...], wd_ref[0, cols, :]).astype(BF16).astype(F32)
            act, dhg, dhu = gate_grads(gate, up, d_act)
            act_ref[:, cols] = act
            dhg_ref[:, cols] = dhg
            dhu_ref[:, cols] = dhu


def outer_kernel(tile_row, tile_exp, half, count, l_ref, r_ref, out_ref, acc, left_t):
    i = pl.program_id(0)
    n = count[0]
    last_step = pl.num_programs(0) - 1
    me = tile_exp[i]
    first = jnp.logical_or(i == 0, tile_exp[jnp.maximum(i - 1, 0)] != me)
    last = jnp.logical_or(i == n - 1, tile_exp[jnp.minimum(i + 1, last_step)] != me)
    live = i < n

    def add(rows):
        left_t[:, :rows] = l_ref[:rows, :].T
        for j in range(acc.shape[1] // COL):
            cols = slice(j * COL, (j + 1) * COL)
            acc[:, cols] += mm(left_t[:, :rows], r_ref[:rows, cols])

    @pl.when(jnp.logical_and(live, first))
    def _():
        acc[...] = jnp.zeros_like(acc)

    @pl.when(jnp.logical_and(live, half[i] == 0))
    def _():
        add(GROUP_TILE)

    @pl.when(jnp.logical_and(live, half[i] == 1))
    def _():
        add(GROUP_TILE // 2)

    @pl.when(jnp.logical_and(live, last))
    def _():
        out_ref[0] = acc[...].astype(BF16)


def spread_kernel(n_chunk, rows, starts, src, dst, buf, in_sem, out_sem):
    def fetch(i):
        at = pl.multiple_of(starts[i], CHUNK_ALIGN)
        return pltpu.make_async_copy(src.at[pl.ds(at, rows), :], buf.at[i], in_sem.at[i])

    def put(i):
        return pltpu.make_async_copy(buf.at[i], dst.at[i], out_sem.at[i])

    for i in range(n_chunk):
        fetch(i).start()
    for i in range(n_chunk):
        fetch(i).wait()
        put(i).start()
    for i in range(n_chunk):
        put(i).wait()


def params():
    return pltpu.CompilerParams(dimension_semantics=("arbitrary",), vmem_limit_bytes=VMEM)


def cost(flops, nbytes):
    return pl.CostEstimate(flops=int(flops), bytes_accessed=int(nbytes), transcendentals=0)


def row_spec(cols, base=0):
    return pl.BlockSpec((ROW_TILE, cols), lambda i, r, e, c: (r[i] + base, 0))


def exp_spec(a, b):
    return pl.BlockSpec((1, a, b), lambda i, r, e, c: (e[i], 0, 0))


def solution(mesh):
    n_dp, n_ep = mesh.shape["dp"], mesh.shape["ep"]
    n_dev = n_dp * n_ep
    all_axes = ("dp", "ep")

    def local_step(hidden, grad_out, expert_ids, norm_gain, w_router, w_gate, w_up, w_down):
        n_tok, width = hidden.shape
        n_exp = w_router.shape[1]
        n_loc, _, ff = w_gate.shape
        capacity = 4 * n_tok // n_exp
        n_choice = 2 * n_tok
        total_tok = n_tok * n_dev
        half_rows = n_loc * n_ep * capacity
        my_dp, my_ep = lax.axis_index("dp"), lax.axis_index("ep")

        x_f32 = hidden.astype(F32)
        inv_rms = lax.rsqrt(jnp.mean(x_f32 * x_f32, axis=-1, keepdims=True) + EPS)
        x_hat = x_f32 * inv_rms
        x_norm = (x_hat * norm_gain).astype(BF16)
        swap = [(i, n_dp - 1 - i) for i in range(n_dp)]
        x_plane = [lax.all_gather(x_norm, "ep", tiled=True)]
        dest_rows, slot_owner = route_tables(expert_ids, n_exp, capacity)
        slots = lax.all_gather(slot_owner.reshape(n_exp, capacity), all_axes)
        dy_plane = [lax.all_gather(grad_out, "ep", tiled=True)]
        x_plane.append(lax.all_gather(lax.ppermute(x_norm, "dp", swap), "ep", tiled=True))
        dy_plane.append(lax.all_gather(lax.ppermute(grad_out, "dp", swap), "ep", tiled=True))

        choice_hot = (expert_ids[:, :, None] == jnp.arange(n_exp, dtype=jnp.int32)).astype(F32)
        xn_f32 = x_norm.astype(F32)
        router_probs = jax.nn.softmax(jnp.dot(xn_f32, w_router, preferred_element_type=F32), axis=-1)
        gate_vals = jnp.sum(router_probs[:, None, :] * choice_hot, axis=-1)
        gate_slots = jnp.zeros((n_exp * capacity,), F32).at[dest_rows].set(gate_vals.reshape(-1))
        gates = lax.all_gather(gate_slots.reshape(n_exp, capacity), all_axes)
        load_frac = jnp.sum((slots < n_choice).astype(F32), axis=(0, 2)) / (2 * total_tok)

        def mine(table):
            table = lax.dynamic_slice(table, (0, n_loc * my_ep, 0), (n_dev, n_loc, capacity))
            planes = table.reshape(n_dp, n_ep, n_loc, capacity)
            return jnp.where(my_dp == 0, planes, planes[::-1])

        my_slots = mine(slots)
        load = jnp.sum((my_slots < n_choice).astype(jnp.int32), axis=-1).transpose(0, 2, 1)
        room = (load + CHUNK_ALIGN - 1) // CHUNK_ALIGN * CHUNK_ALIGN
        chunk_at = jnp.cumsum(room, axis=2) - room
        group_rows = jnp.sum(room, axis=2)
        n_small = (group_rows + ROW_TILE - 1) // ROW_TILE
        n_small = jnp.maximum(n_small, jnp.array([[1], [0]], jnp.int32))
        n_big = (n_small + 1) // 2
        big_at = jnp.cumsum(n_big, axis=1) - n_big
        group_at = big_at * GROUP_TILE + jnp.arange(n_dp, dtype=jnp.int32)[:, None] * half_rows
        row_at = (group_at[:, :, None] + chunk_at).transpose(0, 2, 1).reshape(-1)
        pack_lists = (row_at.reshape(n_dp, -1), room.transpose(0, 2, 1).reshape(n_dp, -1), group_at + group_rows, n_small * ROW_TILE - group_rows)
        slot_token = (my_slots // 2).reshape(n_dev, n_loc, capacity, 1)

        def pack(half, first_list, table, gate, before, name):
            scaled, carry = gate is not None, before is not None
            lists = [jnp.arange(n_ep, dtype=jnp.int32), first_list[half]] + [v[half] for v in pack_lists[1:]]
            part = slice(half * n_ep, (half + 1) * n_ep)
            col_spec = pl.BlockSpec((1, n_loc, capacity, 1), lambda i, *_: (i, 0, 0, 0))
            return pl.pallas_call(
                functools.partial(pack_kernel, scaled, carry, n_loc),
                out_shape=jax.ShapeDtypeStruct((n_dp * half_rows, width), BF16),
                grid_spec=pltpu.PrefetchScalarGridSpec(
                    num_scalar_prefetch=5,
                    grid=(n_ep,),
                    in_specs=[col_spec] * (1 + scaled) + [pl.BlockSpec((n_tok, width), lambda i, s, *_: (s[i], 0))] + [pl.BlockSpec(memory_space=pl.ANY)] * carry,
                    out_specs=pl.BlockSpec(memory_space=pl.ANY),
                    scratch_shapes=[
                        pltpu.VMEM((ROW_TILE, n_tok), BF16),
                        pltpu.VMEM((2, ROW_TILE, width), BF16),
                        pltpu.VMEM((ROW_TILE, width), BF16),
                        pltpu.SemaphoreType.DMA((2,)),
                        pltpu.SemaphoreType.DMA,
                    ],
                ),
                input_output_aliases={7 + scaled: 0} if carry else {},
                compiler_params=params(),
                cost_estimate=cost(2 * n_ep * n_loc * capacity * n_tok * width, 2 * n_ep * n_tok * width),
                name=name,
            )(*lists, slot_token[part], *([gate[part]] if scaled else []), table, *([before] if carry else []))

        slot_gate = mine(gates).reshape(n_dev, n_loc, capacity, 1)
        early_at, slot_gate = lax.optimization_barrier((pack_lists[0], slot_gate))
        x_own = pack(0, early_at, x_plane[0], None, None, "pack_x_own")
        do_own = pack(0, early_at, dy_plane[0], slot_gate, None, "pack_do_own")

        n_step = half_rows // ROW_TILE

        def small_tiles(h):
            ends = jnp.cumsum(n_small[h])
            i = jnp.minimum(jnp.arange(n_step, dtype=jnp.int32), jnp.maximum(ends[-1] - 1, 0))
            e = jnp.minimum(jnp.sum((i[None, :] >= ends[:, None]).astype(jnp.int32), axis=0), n_loc - 1)
            pick = (e[None, :] == jnp.arange(n_loc, dtype=jnp.int32)[:, None]).astype(jnp.int32)
            first = jnp.sum(pick * (2 * big_at[h] - ends + n_small[h])[:, None], axis=0)
            return first + i, e, ends[-1:]

        def big_tiles():
            n = n_big.T.reshape(-1)
            ends = jnp.cumsum(n)
            at = (big_at + jnp.arange(n_dp, dtype=jnp.int32)[:, None] * (half_rows // GROUP_TILE)).T.reshape(-1)
            i = jnp.minimum(jnp.arange(n_step, dtype=jnp.int32), ends[-1] - 1)
            q = jnp.sum((i[None, :] >= ends[:, None]).astype(jnp.int32), axis=0)
            pick = (q[None, :] == jnp.arange(n_dp * n_loc, dtype=jnp.int32)[:, None]).astype(jnp.int32)
            j = i - jnp.sum(pick * (ends - n)[:, None], axis=0)
            small = jnp.sum(pick * n_small.T.reshape(-1)[:, None], axis=0)
            return jnp.sum(pick * at[:, None], axis=0) + j, q // n_dp, (small - 2 * j < 2).astype(jnp.int32), ends[-1:]

        own_tiles, other_tiles, sum_tiles = small_tiles(0), small_tiles(1), big_tiles()
        all_rows = n_dp * half_rows
        wide = jax.ShapeDtypeStruct((all_rows, ff), BF16)
        mat_flops = half_rows * width * ff
        w_bytes = 2 * n_loc * width * ff

        h_gate, h_up, out_rows = pl.pallas_call(
            fwd_kernel,
            out_shape=(jax.ShapeDtypeStruct((half_rows, ff), BF16),) * 2 + (jax.ShapeDtypeStruct((half_rows + capacity, width), BF16),),
            grid_spec=pltpu.PrefetchScalarGridSpec(
                num_scalar_prefetch=3,
                grid=(n_step,),
                in_specs=[row_spec(width), exp_spec(width, ff), exp_spec(width, ff), exp_spec(ff, width)],
                out_specs=[row_spec(ff), row_spec(ff), row_spec(width)],
                scratch_shapes=[pltpu.VMEM((ROW_TILE, ff), BF16)],
            ),
            compiler_params=params(),
            cost_estimate=cost(3 * mat_flops, 3 * w_bytes + half_rows * (2 * ff + 2 * width)),
            name="expert_fwd",
        )(*own_tiles, x_own, w_gate, w_up, w_down)

        n_chunk = n_ep * n_loc
        starts = (big_at[0][:, None] * GROUP_TILE + chunk_at[0]).T.reshape(-1)

        def send_back(rows, name):
            packed = pl.pallas_call(
                functools.partial(spread_kernel, n_chunk, capacity),
                out_shape=jax.ShapeDtypeStruct((n_chunk, capacity, width), BF16),
                grid_spec=pltpu.PrefetchScalarGridSpec(
                    num_scalar_prefetch=1,
                    grid=(),
                    in_specs=[pl.BlockSpec(memory_space=pl.ANY)],
                    out_specs=pl.BlockSpec(memory_space=pl.ANY),
                    scratch_shapes=[pltpu.VMEM((n_chunk, capacity, width), BF16), pltpu.SemaphoreType.DMA((n_chunk,)), pltpu.SemaphoreType.DMA((n_chunk,))],
                ),
                compiler_params=pltpu.CompilerParams(vmem_limit_bytes=VMEM),
                cost_estimate=cost(1e9, 4 * half_rows * width),
                name=name,
            )(starts, rows)
            return lax.all_to_all(packed, "ep", 0, 0, tiled=True).reshape(n_exp * capacity, width)

        back_rows = send_back(out_rows, "pack_out")

        act_rows, d_hgate, d_hup, dx_rows = pl.pallas_call(
            bwd_kernel,
            out_shape=(wide, wide, wide, jax.ShapeDtypeStruct((half_rows + capacity, width), BF16)),
            grid_spec=pltpu.PrefetchScalarGridSpec(
                num_scalar_prefetch=3,
                grid=(n_step,),
                in_specs=[row_spec(ff), row_spec(ff), row_spec(width), exp_spec(width, ff), exp_spec(width, ff), exp_spec(ff, width)],
                out_specs=[row_spec(ff), row_spec(ff), row_spec(ff), row_spec(width)],
            ),
            compiler_params=params(),
            cost_estimate=cost(3 * mat_flops, 3 * w_bytes + half_rows * (5 * ff + 2 * width)),
            name="expert_bwd",
        )(*own_tiles, h_gate, h_up, do_own, w_gate, w_up, w_down)

        d_back = send_back(dx_rows, "pack_dx")

        x_rows = pack(1, early_at, x_plane[1], None, x_own, "pack_x_other")
        do_rows = pack(1, early_at, dy_plane[1], slot_gate, do_own, "pack_do_other")

        any_spec = pl.BlockSpec(memory_space=pl.ANY)
        act_rows, d_hgate, d_hup = pl.pallas_call(
            both_kernel,
            out_shape=(wide, wide, wide),
            grid_spec=pltpu.PrefetchScalarGridSpec(
                num_scalar_prefetch=3,
                grid=(n_step,),
                in_specs=[row_spec(width, n_step), row_spec(width, n_step), exp_spec(width, ff), exp_spec(width, ff), exp_spec(ff, width), any_spec, any_spec, any_spec],
                out_specs=[row_spec(ff, n_step)] * 3,
            ),
            input_output_aliases={8: 0, 9: 1, 10: 2},
            compiler_params=params(),
            cost_estimate=cost(3 * mat_flops, 3 * w_bytes + half_rows * (3 * ff + 2 * width)),
            name="expert_other",
        )(*other_tiles, x_rows, do_rows, w_gate, w_up, w_down, act_rows, d_hgate, d_hup)

        def outer(tiles, left, right, name):
            a, b = left.shape[1], right.shape[1]

            def spec(cols):
                return pl.BlockSpec((GROUP_TILE, cols), lambda i, r, e, h, c: (r[i], 0))

            return pl.pallas_call(
                outer_kernel,
                out_shape=jax.ShapeDtypeStruct((n_loc, a, b), BF16),
                grid_spec=pltpu.PrefetchScalarGridSpec(
                    num_scalar_prefetch=4,
                    grid=(n_step,),
                    in_specs=[spec(a), spec(b)],
                    out_specs=pl.BlockSpec((1, a, b), lambda i, r, e, h, c: (e[i], 0, 0)),
                    scratch_shapes=[pltpu.VMEM((a, b), F32), pltpu.VMEM((a, GROUP_TILE), BF16)],
                ),
                compiler_params=params(),
                cost_estimate=cost(2 * mat_flops, w_bytes + all_rows * (a + b)),
                name=name,
            )(*tiles, left, right)

        g_down = outer(sum_tiles, act_rows, do_rows, "grad_down")

        dest = dest_rows.reshape(n_tok, 2)
        picked = [jnp.take(back_rows, dest[:, j], axis=0, mode="clip").astype(F32) for j in range(2)]
        out_hidden = (x_f32 + (gate_vals[:, :1] * picked[0] + gate_vals[:, 1:] * picked[1])).astype(BF16)
        dy_f32 = grad_out.astype(F32)
        d_gates = [jnp.sum(dy_f32 * p, axis=-1, keepdims=True) for p in picked]
        d_probs = d_gates[0] * choice_hot[:, 0] + d_gates[1] * choice_hot[:, 1] + (AUX_COEF * n_exp / total_tok) * load_frac
        d_logits = router_probs * (d_probs - jnp.sum(router_probs * d_probs, axis=-1, keepdims=True))
        d_taken = [jnp.take(d_back, dest[:, j], axis=0, mode="clip").astype(F32) for j in range(2)]
        d_xnorm = jnp.einsum("te,de->td", d_logits, w_router) + d_taken[0] + d_taken[1]
        d_xnorm = d_xnorm.astype(BF16).astype(F32)
        scaled = d_xnorm * norm_gain
        grad_hidden = (inv_rms * (scaled - x_hat * jnp.mean(scaled * x_hat, axis=-1, keepdims=True)) + dy_f32).astype(BF16)
        g_gain = jnp.sum(d_xnorm * x_hat, axis=0)
        g_router = jnp.einsum("td,te->de", xn_f32, d_logits)
        prob_sum = jnp.pad(jnp.sum(router_probs, axis=0), (0, width - n_exp))
        count, small_sums = lax.optimization_barrier((sum_tiles[3], jnp.concatenate([g_router, g_gain[:, None], prob_sum[:, None]], axis=1)))
        small_sums = lax.psum(small_sums, all_axes)
        g_router, g_gain, prob_sum = small_sums[:, :n_exp], small_sums[:, n_exp], small_sums[:n_exp, n_exp + 1]
        g_gate = outer((*sum_tiles[:3], count), x_rows, d_hgate, "grad_gate")
        g_up = outer((*sum_tiles[:3], count), x_rows, d_hup, "grad_up")
        aux_loss = AUX_COEF * n_exp * jnp.sum(load_frac * prob_sum / total_tok)
        return (out_hidden, aux_loss, grad_hidden, g_gain, g_router, g_gate, g_up, g_down)

    tok_spec = P(all_axes, None)
    w_spec = P("ep", None, None)
    return jax.shard_map(local_step, mesh=mesh, in_specs=(tok_spec, tok_spec, tok_spec, P(), P(), w_spec, w_spec, w_spec), out_specs=(tok_spec, P(), tok_spec, P(), P(), w_spec, w_spec, w_spec), check_vma=False)
```
